32 devices in a mesh: mem: 4 (over y, core), tile: 8 (over z, x).
Axes of the slice: x: 2, y: 2, z: 4, core: 2. Of those that a mesh axis runs over, the one named last changes fastest.
Arguments:
- ensemble_profiles_before: bfloat16 [64, 40, 4096], P('mem', None, 'tile'), may hold values from -6 to 6
- mixing_coefficient: float32 [4096], P('tile'), may hold values from 0.05 to 0.24
- surface_driver: float32 [64, 4096], P('mem', 'tile'), may hold values from -3 to 3
- terrain_indicator: int32 [4096], P('tile'), may hold values 0 or 1
- measured_profile_position: int32 [32768], P('tile'), may hold values from 0 to 511
- measured_field_index: int32 [32768], P('tile'), may hold values from 0 to 39
- obs_valid: int32 [32768], P('tile'), may hold values 0 or 1
- obs_value: bfloat16 [32768], P('tile'), may hold values from -6 to 6
- obs_error: bfloat16 [32768], P('tile'), may hold values from 0.5 to 4
- local_weight: float32 [4, 8, 20480], P('mem', 'tile'), may hold values from 0.001 to 0.03
Outputs:
- analysis: bfloat16 [64, 40, 4096], P('mem', None, 'tile')
The draws below stay inside these ranges and needn't reach their ends.
All inputs are finite; a program needn't handle non-finite values. No bound on the sum of `terrain_indicator` or of `obs_valid` on one device may be relied on, other than what follows from the above.
Results may differ from the reference program's by a relative error of at most 0.0034.
Values may be sent and summed in bfloat16 or wider, within the bound.
A program may use at most 64 MiB of HBM per device.

```python
import math
import jax
import jax.numpy as jnp
from jax import lax

K = 64
PROFILE_SIZE = 40
BLK = 128
OBS_T = 4096
REACH = 2
NS_ITERS = 3
C_TILE = 512
COLS = 4096
NB_TILE = 4
P_OBS = 20480
N_TILE = 8


def set_ends(values, stream_key, least, largest):
    longest = values.shape.index(max(values.shape))
    spots = []
    for shift in (0, 1):
        where = [jax.random.randint(jax.random.fold_in(stream_key, axis), (), 0, length) for axis, length in enumerate(values.shape)]
        where[longest] = (where[longest] + shift) % values.shape[longest]
        spots.append(tuple(where))
    return values.at[spots[0]].set(least).at[spots[1]].set(largest)


def block_levels(rng, extent, pieces, least, high):
    level, own = 1.0, jax.random.fold_in(rng, 6)
    for position, blocks in pieces:
        steps = jnp.exp(jax.random.uniform(jax.random.fold_in(own, position), (blocks,), jnp.float32, least / len(pieces), high / len(pieces)))
        level = level * jnp.repeat(steps, extent[position] // blocks).reshape([-1 if axis == position else 1 for axis in range(len(extent))])
    return level


def centred(key, shape, scale, reach, cuts=(), kind=jnp.bfloat16):
    values = scale * jax.random.normal(key, shape, jnp.float32)
    if cuts:
        values = values * block_levels(key, shape, cuts, -0.22, 0.18)
    return jnp.clip(values, -reach, reach).astype(kind)


def setup_inputs(seed: int = 0) -> dict:
    arg_keys = jax.random.split(jax.random.key(seed), 11)
    return {
        "ensemble_profiles_before": centred(arg_keys[0], (K, PROFILE_SIZE, COLS), 1.0, 6.0, ((0, 4), (2, 8))),
        "mixing_coefficient": jnp.clip(jnp.exp(math.log(0.24) - 1.5686159 * jax.random.uniform(arg_keys[1], (COLS,), jnp.float32) ** block_levels(arg_keys[1], (COLS,), ((0, 8),), -0.2, 0.2)), 0.05, 0.24),
        "surface_driver": centred(arg_keys[2], (K, COLS), 0.5, 3.0, ((0, 4), (1, 8)), jnp.float32),
        "terrain_indicator": set_ends((jax.random.randint(arg_keys[3], (COLS,), 0, 4) < 3).astype(jnp.int32), jax.random.fold_in(arg_keys[3], 1), 0, 1),
        "measured_profile_position": set_ends(jax.random.randint(arg_keys[4], (N_TILE * OBS_T,), 0, C_TILE), jax.random.fold_in(arg_keys[4], 1), 0, C_TILE - 1).astype(jnp.int32),
        "measured_field_index": set_ends(jax.random.randint(arg_keys[5], (N_TILE * OBS_T,), 0, PROFILE_SIZE), jax.random.fold_in(arg_keys[5], 1), 0, PROFILE_SIZE - 1).astype(jnp.int32),
        "obs_valid": set_ends((jax.random.randint(arg_keys[6], (N_TILE * OBS_T,), 0, 8) < 7).astype(jnp.int32), jax.random.fold_in(arg_keys[6], 1), 0, 1),
        "obs_value": centred(arg_keys[7], (N_TILE * OBS_T,), 1.0, 6.0, ((0, 8),)),
        "obs_error": jnp.clip(jnp.exp(math.log(4.0) - 2.0794415 * jax.random.uniform(arg_keys[8], (N_TILE * OBS_T,), jnp.float32) ** block_levels(arg_keys[8], (N_TILE * OBS_T,), ((0, 8),), -0.2, 0.2)), 0.5, 4.0).astype(jnp.bfloat16),
        "local_weight": jnp.clip(jnp.exp(math.log(0.03) - 3.4011973 * jax.random.uniform(arg_keys[9], (NB_TILE, N_TILE, P_OBS), jnp.float32) ** block_levels(arg_keys[9], (NB_TILE, N_TILE, P_OBS), ((0, 4), (1, 8)), -0.2, 0.2)), 0.001, 0.03),
    }


EXACT = lax.Precision.HIGHEST

def vertical_mixing_step(ensemble_profiles_before, mixing_coefficient, surface_driver, terrain_indicator):
    values = ensemble_profiles_before.astype(jnp.float32)
    above_layer = jnp.concatenate([values[:, :1], values[:, :-1]], axis=1)
    below_layer = jnp.concatenate([values[:, 1:], values[:, -1:]], axis=1)
    diffused = values + mixing_coefficient[None, None, :] * (above_layer - 2.0 * values + below_layer)
    stepped = diffused - 0.05 * values * values * values
    surface = jnp.concatenate([stepped[:, :1] + surface_driver[:, None, :], stepped[:, 1:]], axis=1)
    result = jnp.where(terrain_indicator[None, None, :] > 0, surface, values)
    return result.astype(jnp.bfloat16)

def measurement_operator(background_ensemble, measured_profile_position, measured_field_index):
    profile_sequence = background_ensemble.shape[2]
    unrolled_ensemble = background_ensemble.reshape(background_ensemble.shape[0], -1)
    slot_index = measured_field_index.astype(jnp.int32) * profile_sequence + measured_profile_position.astype(jnp.int32)
    return jnp.take(unrolled_ensemble, slot_index, axis=1)

def prepare(window):
    ensemble_profiles = window.shape[0] - 3
    measured_quantities = window[:ensemble_profiles].astype(jnp.float32)
    average = lax.optimization_barrier(jnp.mean(measured_quantities, axis=0))
    deviation = measured_quantities - average
    innovation = window[ensemble_profiles].astype(jnp.float32) - average
    obs_precision = window[ensemble_profiles + 2].astype(jnp.float32) / window[ensemble_profiles + 1].astype(jnp.float32)
    return (deviation, innovation, obs_precision)

def weights_for(deviation, innovation, precision, portions):
    ensemble_profiles = deviation.shape[0]
    portion_width = deviation.shape[1] // portions
    spread = jnp.zeros((ensemble_profiles, ensemble_profiles), jnp.float32)
    for portion_index in range(portions):
        portion = deviation[:, portion_index * portion_width:(portion_index + 1) * portion_width]
        scaled = portion * precision[None, portion_index * portion_width:(portion_index + 1) * portion_width]
        spread = spread + jnp.dot(scaled, portion.T, precision=EXACT, preferred_element_type=jnp.float32)
    spread = spread / (ensemble_profiles - 1.0)
    pulled = jnp.dot(deviation, precision * innovation, precision=EXACT, preferred_element_type=jnp.float32) / (ensemble_profiles - 1.0)
    identity = jnp.eye(ensemble_profiles, dtype=jnp.float32)
    system = identity + spread
    norm_scale = jnp.sqrt(jnp.sum(system * system))

    def newton(sweep, carry):
        current, inv_root = carry
        middle = 1.5 * identity - 0.5 * jnp.dot(inv_root, current, precision=EXACT)
        return (jnp.dot(current, middle, precision=EXACT), jnp.dot(middle, inv_root, precision=EXACT))
    current, inv_root = lax.fori_loop(0, NS_ITERS, newton, (system / norm_scale, identity))
    inv_root = inv_root / jnp.sqrt(norm_scale)
    inverse = jnp.dot(inv_root, inv_root, precision=EXACT)
    mean_weight = jnp.dot(inverse, pulled, precision=EXACT)
    return inv_root + mean_weight[:, None]

def update(states, transform, land_block):
    values = states.astype(jnp.float32)
    average = lax.optimization_barrier(jnp.mean(values, axis=0))
    deviation = values - average[None]
    moved = jnp.einsum('isc,ij->jsc', deviation, transform, precision=EXACT)
    result = jnp.where(land_block[None, None, :] > 0, average[None] + moved, values)
    return result.astype(jnp.bfloat16)

def reference(ensemble_profiles_before, mixing_coefficient, surface_driver, terrain_indicator, measured_profile_position, measured_field_index, obs_valid, obs_value, obs_error, local_weight):
    background_ensemble = vertical_mixing_step(ensemble_profiles_before, mixing_coefficient, surface_driver, terrain_indicator)
    number_sections = N_TILE
    ensemble_profiles = ensemble_profiles_before.shape[0]
    section_breadth = ensemble_profiles_before.shape[2] // number_sections
    blocks_tile = section_breadth // BLK
    sectioned_ensemble = background_ensemble.reshape(ensemble_profiles, PROFILE_SIZE, number_sections, section_breadth).transpose(2, 0, 1, 3)
    measured_quantities = jax.vmap(measurement_operator)(sectioned_ensemble, measured_profile_position.reshape(number_sections, OBS_T), measured_field_index.reshape(number_sections, OBS_T))
    metadata = jnp.stack([obs_value.reshape(number_sections, OBS_T), obs_error.reshape(number_sections, OBS_T), obs_valid.reshape(number_sections, OBS_T).astype(jnp.bfloat16)], axis=1)
    obs_rows = jnp.concatenate([measured_quantities, metadata], axis=1)
    offsets = jnp.arange(-REACH, REACH + 1, dtype=jnp.int32)
    land_tiles = terrain_indicator.reshape(number_sections, blocks_tile, BLK)

    def one_tile(tile_index):
        chosen = (tile_index + offsets) % number_sections
        window = jnp.take(obs_rows, chosen, axis=0).transpose(1, 0, 2).reshape(ensemble_profiles + 3, -1)
        deviation, innovation, obs_precision = prepare(window)
        tile_states = lax.dynamic_index_in_dim(sectioned_ensemble, tile_index, 0, keepdims=False)
        tile_states = tile_states.reshape(ensemble_profiles, PROFILE_SIZE, blocks_tile, BLK).transpose(2, 0, 1, 3)
        tile_land = lax.dynamic_index_in_dim(land_tiles, tile_index, 0, keepdims=False)
        tile_weight = lax.dynamic_index_in_dim(local_weight, tile_index, 1, keepdims=False)

        def one_block(inputs):
            states, land_block, weight = inputs
            transform = weights_for(deviation, innovation, obs_precision * weight, 2 * REACH + 1)
            return update(states, transform, land_block)
        finished = lax.map(one_block, (tile_states, tile_land, tile_weight))
        return finished.transpose(1, 2, 0, 3).reshape(ensemble_profiles, PROFILE_SIZE, section_breadth)
    analysed = lax.map(one_tile, jnp.arange(number_sections, dtype=jnp.int32))
    return analysed.transpose(1, 2, 0, 3).reshape(ensemble_profiles, PROFILE_SIZE, number_sections * section_breadth)
```

```python
import functools

import jax
import jax.numpy as jnp
from jax import lax
from jax.experimental import pallas as pl
from jax.experimental.pallas import tpu as pltpu
from jax.sharding import PartitionSpec as P

REACH = 2
NS_ITERS = 3


EXACT = lax.Precision.HIGHEST


def from_behind(value, axis, steps):
    count = lax.axis_size(axis)
    pairs = [(source, (source + steps) % count) for source in range(count)]
    return lax.ppermute(value, axis, pairs)


def vertical_mixing_step(
    ensemble_profiles_before, mixing_coefficient, surface_driver, terrain_indicator
):
    values = ensemble_profiles_before.astype(jnp.float32)
    above_layer = jnp.concatenate([values[:, :1], values[:, :-1]], axis=1)
    below_layer = jnp.concatenate([values[:, 1:], values[:, -1:]], axis=1)
    diffused = values + mixing_coefficient[None, None, :] * (
        above_layer - 2.0 * values + below_layer
    )
    stepped = diffused - 0.05 * values * values * values
    surface = jnp.concatenate([stepped[:, :1] + surface_driver[:, None, :], stepped[:, 1:]], axis=1)
    result = jnp.where(terrain_indicator[None, None, :] > 0, surface, values)
    return result.astype(jnp.bfloat16)


def measurement_operator(background_ensemble, measured_profile_position, measured_field_index):
    profile_sequence = background_ensemble.shape[2]
    unrolled_ensemble = background_ensemble.reshape(background_ensemble.shape[0], -1)
    slot_index = measured_field_index * profile_sequence + measured_profile_position
    return jnp.take(unrolled_ensemble, slot_index, axis=1)


def prepare(window):
    ensemble_profiles = window.shape[0] - 3
    measured_quantities = window[:ensemble_profiles].astype(jnp.float32)
    average = jnp.mean(measured_quantities, axis=0)
    deviation = measured_quantities - average
    innovation = window[ensemble_profiles].astype(jnp.float32) - average
    obs_precision = window[ensemble_profiles + 2].astype(jnp.float32) / window[
        ensemble_profiles + 1
    ].astype(jnp.float32)
    return (deviation, innovation, obs_precision)


def weights_for(deviation, innovation, precision, portions):
    ensemble_profiles = deviation.shape[0]
    portion_width = deviation.shape[1] // portions
    spread = jnp.zeros((ensemble_profiles, ensemble_profiles), jnp.float32)
    for portion_index in range(portions):
        portion = deviation[:, portion_index * portion_width : (portion_index + 1) * portion_width]
        scaled = (
            portion
            * precision[None, portion_index * portion_width : (portion_index + 1) * portion_width]
        )
        spread = spread + jnp.dot(
            scaled, portion.T, precision=EXACT, preferred_element_type=jnp.float32
        )
    spread = spread / (ensemble_profiles - 1.0)
    pulled = jnp.dot(
        deviation, precision * innovation, precision=EXACT, preferred_element_type=jnp.float32
    ) / (ensemble_profiles - 1.0)
    identity = jnp.eye(ensemble_profiles, dtype=jnp.float32)
    system = identity + spread
    norm_scale = jnp.sqrt(jnp.sum(system * system))

    def newton(sweep, carry):
        current, inv_root = carry
        middle = 1.5 * identity - 0.5 * jnp.dot(inv_root, current, precision=EXACT)
        return (
            jnp.dot(current, middle, precision=EXACT),
            jnp.dot(middle, inv_root, precision=EXACT),
        )

    current, inv_root = lax.fori_loop(0, NS_ITERS, newton, (system / norm_scale, identity))
    inv_root = inv_root / jnp.sqrt(norm_scale)
    inverse = jnp.dot(inv_root, inv_root, precision=EXACT)
    mean_weight = jnp.dot(inverse, pulled, precision=EXACT)
    return inv_root + mean_weight[:, None]


def update(states, transform, land_block):
    values = states.astype(jnp.float32)
    average = jnp.mean(values, axis=0)
    deviation = values - average[None]
    moved = jnp.einsum("isc,ij->jsc", deviation, transform, precision=EXACT)
    result = jnp.where(land_block[None, None, :] > 0, average[None] + moved, values)
    return result.astype(jnp.bfloat16)


def plain_on_device(
    ensemble_profiles_before,
    mixing_coefficient,
    surface_driver,
    terrain_indicator,
    measured_profile_position,
    measured_field_index,
    obs_valid,
    obs_value,
    obs_error,
    local_weight,
):
    background_ensemble = vertical_mixing_step(
        ensemble_profiles_before, mixing_coefficient, surface_driver, terrain_indicator
    )
    measured_quantities = measurement_operator(
        background_ensemble, measured_profile_position, measured_field_index
    )
    metadata = jnp.stack([obs_value, obs_error, obs_valid.astype(jnp.bfloat16)])
    own_rows = jnp.concatenate([measured_quantities, metadata], axis=0)
    pieces = []
    for offset in range(-REACH, REACH + 1):
        if offset == 0:
            pieces.append(own_rows)
        else:
            pieces.append(from_behind(own_rows, "tile", -offset))
    nearby = jnp.concatenate(pieces, axis=1)
    members_here = measured_quantities.shape[0]
    everyone = lax.all_gather(nearby[:members_here], "mem", axis=0, tiled=True)
    window = jnp.concatenate([everyone, nearby[members_here:]], axis=0)
    regrouped_states = lax.all_to_all(
        background_ensemble, "mem", split_axis=2, concat_axis=0, tiled=True
    )
    deviation, innovation, obs_precision = prepare(window)
    columns_here = regrouped_states.shape[2]
    local_land = lax.dynamic_slice_in_dim(
        terrain_indicator, lax.axis_index("mem") * columns_here, columns_here
    )
    transform = weights_for(
        deviation, innovation, obs_precision * local_weight[0, 0], 2 * REACH + 1
    )
    outputs = update(regrouped_states, transform, local_land)
    return lax.all_to_all(outputs, "mem", split_axis=0, concat_axis=2, tiled=True)


MESH = pl.DeviceIdType.MESH
HALVES = 2
FIELD_CUTS = (0.4, 0.7)
CORES = 2


def exact_dot(a, b):
    return jnp.dot(a, b, precision=EXACT, preferred_element_type=jnp.float32)


def kernel(
    n_mem,
    n_tile,
    cuts,
    ens_ref,
    mix_ref,
    surf_ref,
    land_ref,
    pos_ref,
    field_ref,
    valid_ref,
    value_ref,
    error_ref,
    weight_ref,
    out_ref,
    fc_ref,
    seen_ref,
    near_ref,
    rinv_ref,
    part_ref,
    got_ref,
    tsend_ref,
    trecv_ref,
    moved_ref,
    seen_send,
    seen_recv,
    fc_send,
    fc_recv,
    w_send,
    w_recv,
    p_send,
    p_recv,
    t_send,
    t_recv,
):
    members, fields, columns = ens_ref.shape
    everyone = members * n_mem
    slots = pos_ref.shape[1]
    near = 2 * REACH + 1
    me, tile = lax.axis_index("mem"), lax.axis_index("tile")
    n_y = n_mem // CORES
    y, core = me // CORES, lax.rem(me, CORES)
    sibling = y * CORES + (1 - core)
    across = [lax.rem(y + step, n_y) * CORES + core for step in range(1, n_y)]
    partner_of = [lax.rem(y + step, n_y) * CORES + (1 - core) for step in range(1, n_y)]

    barrier = pltpu.get_barrier_semaphore()
    for step in range(1, n_mem):
        pl.semaphore_signal(
            barrier, inc=1, device_id={"mem": lax.rem(me + step, n_mem)}, device_id_type=MESH
        )
    for offset in range(-REACH, REACH + 1):
        if offset:
            pl.semaphore_signal(
                barrier,
                inc=1,
                device_id={"tile": lax.rem(tile + offset + n_tile, n_tile)},
                device_id_type=MESH,
            )

    lanes = 128

    def mix(step, carry):
        where = pl.ds(pl.multiple_of(step * lanes, lanes), lanes)
        x = jnp.transpose(ens_ref[:, :, where].astype(jnp.float32), (1, 0, 2))
        rate = mix_ref[:, where][None]
        above = jnp.concatenate([x[:1], x[:-1]], axis=0)
        below = jnp.concatenate([x[1:], x[-1:]], axis=0)
        stepped = x + rate * (above - 2.0 * x + below) - 0.05 * x * x * x
        top = stepped[:1] + surf_ref[:, where][None]
        stepped = jnp.concatenate([top, stepped[1:]], axis=0)
        land = jnp.broadcast_to(land_ref[:, where][None], x.shape) > 0
        fc_ref[me, :, :, where] = jnp.where(land, stepped, x).astype(jnp.bfloat16)
        return carry

    lax.fori_loop(0, columns // lanes, mix, 0)
    pl.semaphore_wait(barrier, n_mem - 1 + 2 * REACH)

    def remote(src, dst, send, recv, where):
        return pltpu.make_async_remote_copy(
            src_ref=src,
            dst_ref=dst,
            send_sem=send,
            recv_sem=recv,
            device_id=where,
            device_id_type=MESH,
        )

    started = []

    def go(copy):
        copy.start()
        started.append(copy)

    def weight_copy(j):
        return remote(
            weight_ref.at[j],
            near_ref.at[j],
            w_send.at[j],
            w_recv.at[j],
            {"tile": lax.rem(tile + j - REACH + n_tile, n_tile)},
        )

    def fc_copy(q, owner, lane, target):
        block = fc_ref.at[owner, pl.ds(cuts[q], cuts[q + 1] - cuts[q])]
        return remote(block, block, fc_send.at[q, lane], fc_recv.at[q, owner], {"mem": target})

    def seen_copy(h, owner, lane, target):
        block = seen_ref.at[owner, h]
        return remote(
            block, block, seen_send.at[h, lane], seen_recv.at[h, owner], {"mem": target}
        )

    def own_fc(q):
        for index, peer in enumerate(across):
            go(fc_copy(q, me, index, peer))
        go(fc_copy(q, me, n_y - 1, sibling))

    def relay_fc(q):
        for index, peer in enumerate(across):
            fc_copy(q, peer, index, peer).wait_recv()
            go(fc_copy(q, peer, n_y + index, sibling))

    for j in range(near):
        if j != REACH:
            go(weight_copy(j))
    own_fc(0)

    half = slots // HALVES
    width = min(half, 512)
    for h in range(HALVES):

        def pick(step, carry, h=h):
            inner = pl.ds(pl.multiple_of(step * width, width), width)
            where = pl.ds(pl.multiple_of(h * half + step * width, width), width)
            rows = lax.broadcasted_iota(jnp.int32, (columns, width), 0)
            hot = jnp.where(rows == pos_ref[:, where], 1.0, 0.0).astype(jnp.bfloat16)
            flat = fc_ref[me].reshape(fields * members, columns)
            found = jnp.dot(flat, hot, preferred_element_type=jnp.float32)
            wanted = jnp.broadcast_to(field_ref[:, where], (members, width))
            total = found[:members]
            for f in range(1, fields):
                total = jnp.where(wanted == f, found[f * members : (f + 1) * members], total)
            seen_ref[me, h, :, inner] = total.astype(jnp.bfloat16)
            return carry

        lax.fori_loop(0, half // width, pick, 0)
        for index, peer in enumerate(across):
            go(seen_copy(h, me, index, peer))
        go(seen_copy(h, me, n_y - 1, sibling))

    n_cuts = len(cuts) - 1
    for q in range(1, n_cuts):
        own_fc(q)

    base = valid_ref[...].astype(jnp.float32) / error_ref[...].astype(jnp.float32)
    rinv_ref[...] = jnp.zeros_like(rinv_ref)
    for j in range(near):
        if j == REACH:
            rinv_ref[j : j + 1, :] = base * weight_ref[j]
        else:
            weight_copy(j).wait_recv()
            rinv_ref[j : j + 1, :] = base * near_ref[j]
    part_ref[...] = jnp.zeros_like(part_ref)

    for h in range(HALVES):
        for index, peer in enumerate(across):
            seen_copy(h, peer, index, peer).wait_recv()
            go(seen_copy(h, peer, n_y + index, sibling))
    for h in range(HALVES):
        for owner in [sibling, *partner_of]:
            seen_copy(h, owner, 0, sibling).wait_recv()

        def gather_stats(step, carry, h=h):
            inner = pl.ds(pl.multiple_of(step * width, width), width)
            where = pl.ds(pl.multiple_of(h * half + step * width, width), width)
            seen = jnp.concatenate(
                [seen_ref[m, h, :, inner].astype(jnp.float32) for m in range(n_mem)], axis=0
            )
            average = jnp.mean(seen, axis=0, keepdims=True)
            deviation = seen - average
            innovation = value_ref[:, where].astype(jnp.float32) - average
            rinv = rinv_ref[:, where]
            high = deviation.astype(jnp.bfloat16)
            low = (deviation - high.astype(jnp.float32)).astype(jnp.bfloat16)
            right = jnp.concatenate([high, low], axis=0)
            pulls = rinv * innovation
            rows = [(deviation * rinv[j : j + 1]).astype(jnp.bfloat16) for j in range(near)]
            rows.append(jnp.concatenate([pulls, jnp.zeros_like(pulls)], axis=0).astype(jnp.bfloat16))
            left = jnp.concatenate(rows, axis=0)
            sums = lax.dot_general(
                left, right, (((1,), (1,)), ((), ())), preferred_element_type=jnp.float32
            )
            for j in range(near):
                part_ref[j, :everyone] += sums[j * everyone : (j + 1) * everyone]
                part_ref[j, everyone:] += jnp.broadcast_to(
                    sums[near * everyone + j : near * everyone + j + 1], (8, 2 * everyone)
                )
            return carry

        lax.fori_loop(0, half // width, gather_stats, 0)

    def part_copy(j):
        return remote(
            part_ref.at[j],
            got_ref.at[j],
            p_send.at[j],
            p_recv.at[j],
            {"tile": lax.rem(tile - (j - REACH) + n_tile, n_tile)},
        )

    for j in range(near):
        if j != REACH:
            go(part_copy(j))
    for q in range(n_cuts - 1):
        relay_fc(q)
    summed = part_ref[REACH]
    for j in range(near):
        if j != REACH:
            part_copy(j).wait_recv()
            summed = summed + got_ref[j]
    summed = (summed[:, :everyone] + summed[:, everyone:]) / (everyone - 1.0)
    rows = lax.broadcasted_iota(jnp.int32, (everyone, everyone), 0)
    identity = jnp.where(
        rows == lax.broadcasted_iota(jnp.int32, (everyone, everyone), 1), 1.0, 0.0
    )
    system = identity + summed[:everyone]
    pulled = summed[everyone:]
    scale = jnp.sqrt(jnp.sum(system * system, keepdims=True))
    current = system / scale
    root = 1.5 * identity - 0.5 * current
    current = exact_dot(current, root)
    for sweep in range(1, NS_ITERS):
        middle = 1.5 * identity - 0.5 * exact_dot(root, current)
        if sweep < NS_ITERS - 1:
            current = exact_dot(current, middle)
        root = exact_dot(middle, root)
    root = root / jnp.sqrt(scale)
    mean_weight = exact_dot(exact_dot(pulled, root), root)[:1]
    turned = root + mean_weight
    turned = turned + (1.0 - jnp.sum(turned, axis=1, keepdims=True)) / everyone
    for m in range(n_mem):
        tsend_ref[m, :, :everyone] = turned[m * members : (m + 1) * members]
        tsend_ref[m, :, everyone:] = jnp.zeros((members, everyone), jnp.float32)

    def t_copy(owner, target, lane):
        return remote(
            tsend_ref.at[target],
            trecv_ref.at[owner],
            t_send.at[lane],
            t_recv.at[owner],
            {"mem": target},
        )

    for step in range(1, n_mem):
        go(t_copy(me, lax.rem(me + step, n_mem), step))
    trecv_ref[me] = tsend_ref[me]
    relay_fc(n_cuts - 1)
    for q in range(n_cuts):
        for owner in [sibling, *partner_of]:
            fc_copy(q, owner, 0, sibling).wait_recv()
    for step in range(1, n_mem):
        t_copy(lax.rem(me + step, n_mem), me, step).wait_recv()

    wide = columns // n_mem
    group = 8

    def apply(block, carry):
        where = pl.ds(pl.multiple_of(block * wide, wide), wide)
        weights = trecv_ref[block][:, :everyone]
        high = weights.astype(jnp.bfloat16)
        low = (weights - high.astype(jnp.float32)).astype(jnp.bfloat16)
        left = jnp.concatenate([high, low], axis=0)
        land = jnp.broadcast_to(land_ref[:, where], (members, wide)) > 0
        for first in range(0, fields, group):
            states = jnp.concatenate(
                [
                    jnp.concatenate([fc_ref[m, f, :, where] for m in range(n_mem)], axis=0)
                    for f in range(first, first + group)
                ],
                axis=1,
            )
            both = jnp.dot(left, states, preferred_element_type=jnp.float32)
            total = both[:members] + both[members:]
            for f in range(group):
                moved_ref[first + f, :, :] = jnp.where(
                    land,
                    total[:, f * wide : (f + 1) * wide],
                    fc_ref[me, first + f, :, where].astype(jnp.float32),
                )
        out_ref[:, :, where] = jnp.transpose(moved_ref[...], (1, 0, 2)).astype(jnp.bfloat16)
        return carry

    lax.fori_loop(0, n_mem, apply, 0)
    for copy in started:
        copy.wait_send()


def on_device(
    n_mem,
    n_tile,
    ensemble_profiles_before,
    mixing_coefficient,
    surface_driver,
    terrain_indicator,
    measured_profile_position,
    measured_field_index,
    obs_valid,
    obs_value,
    obs_error,
    local_weight,
):
    members, fields, columns = ensemble_profiles_before.shape
    slots = measured_field_index.shape[0]
    everyone = members * n_mem
    near = 2 * REACH + 1
    n_y = n_mem // CORES
    cuts = (0, *[int(fields * cut) for cut in FIELD_CUTS], fields)
    n_cuts = len(cuts) - 1
    row = lambda a: a.reshape(1, -1)
    whole = pl.BlockSpec(memory_space=pltpu.VMEM)
    dma = pltpu.SemaphoreType.DMA
    return pl.pallas_call(
        functools.partial(kernel, n_mem, n_tile, cuts),
        out_shape=jax.ShapeDtypeStruct(ensemble_profiles_before.shape, jnp.bfloat16),
        in_specs=[whole] * 10,
        out_specs=whole,
        scratch_shapes=[
            pltpu.VMEM((n_mem, fields, members, columns), jnp.bfloat16),
            pltpu.VMEM((n_mem, HALVES, members, slots // HALVES), jnp.bfloat16),
            pltpu.VMEM((near, 1, slots), jnp.float32),
            pltpu.VMEM((8, slots), jnp.float32),
            pltpu.VMEM((near, everyone + 8, 2 * everyone), jnp.float32),
            pltpu.VMEM((near, everyone + 8, 2 * everyone), jnp.float32),
            pltpu.VMEM((n_mem, members, 2 * everyone), jnp.float32),
            pltpu.VMEM((n_mem, members, 2 * everyone), jnp.float32),
            pltpu.VMEM((fields, members, columns // n_mem), jnp.float32),
            dma((HALVES, 2 * n_y)),
            dma((HALVES, n_mem)),
            dma((n_cuts, 2 * n_y)),
            dma((n_cuts, n_mem)),
            dma((near,)),
            dma((near,)),
            dma((near,)),
            dma((near,)),
            dma((n_mem,)),
            dma((n_mem,)),
        ],
        compiler_params=pltpu.CompilerParams(
            collective_id=0, has_side_effects=True, vmem_limit_bytes=48 * 2**20
        ),
    )(
        ensemble_profiles_before,
        row(mixing_coefficient),
        surface_driver,
        row(terrain_indicator),
        row(measured_profile_position),
        row(measured_field_index),
        row(obs_valid),
        row(obs_value),
        row(obs_error),
        local_weight.reshape(near, 1, slots),
    )


def fits(n_mem, n_tile, ensemble, slots):
    members, fields, columns = ensemble[0] // n_mem, ensemble[1], ensemble[2] // n_tile
    return (
        n_mem % CORES == 0
        and n_tile > 2 * REACH
        and members % 16 == 0
        and fields % 8 == 0
        and columns % (128 * n_mem) == 0
        and slots // n_tile % (512 * HALVES) == 0
    )


def solution(mesh):
    in_specs = (
        P("mem", None, "tile"),
        P("tile"),
        P("mem", "tile"),
        P("tile"),
        P("tile"),
        P("tile"),
        P("tile"),
        P("tile"),
        P("tile"),
        P("mem", "tile", None),
    )
    out_specs = P("mem", None, "tile")

    def run(*args):
        sizes = mesh.shape["mem"], mesh.shape["tile"]
        body = plain_on_device
        if fits(*sizes, args[0].shape, args[5].shape[0]):
            body = functools.partial(on_device, *sizes)
        return jax.shard_map(
            body, mesh=mesh, in_specs=in_specs, out_specs=out_specs, check_vma=False
        )(*args)

    return run
```

```python
import functools

import jax
import jax.numpy as jnp
from jax import lax
from jax.experimental import pallas as pl
from jax.experimental.pallas import tpu as pltpu
from jax.sharding import PartitionSpec as P

REACH = 2
NS_ITERS = 3


EXACT = lax.Precision.HIGHEST


def from_behind(value, axis, steps):
    count = lax.axis_size(axis)
    pairs = [(source, (source + steps) % count) for source in range(count)]
    return lax.ppermute(value, axis, pairs)


def vertical_mixing_step(
    ensemble_profiles_before, mixing_coefficient, surface_driver, terrain_indicator
):
    values = ensemble_profiles_before.astype(jnp.float32)
    above_layer = jnp.concatenate([values[:, :1], values[:, :-1]], axis=1)
    below_layer = jnp.concatenate([values[:, 1:], values[:, -1:]], axis=1)
    diffused = values + mixing_coefficient[None, None, :] * (
        above_layer - 2.0 * values + below_layer
    )
    stepped = diffused - 0.05 * values * values * values
    surface = jnp.concatenate([stepped[:, :1] + surface_driver[:, None, :], stepped[:, 1:]], axis=1)
    result = jnp.where(terrain_indicator[None, None, :] > 0, surface, values)
    return result.astype(jnp.bfloat16)


def measurement_operator(background_ensemble, measured_profile_position, measured_field_index):
    profile_sequence = background_ensemble.shape[2]
    unrolled_ensemble = background_ensemble.reshape(background_ensemble.shape[0], -1)
    slot_index = measured_field_index * profile_sequence + measured_profile_position
    return jnp.take(unrolled_ensemble, slot_index, axis=1)


def prepare(window):
    ensemble_profiles = window.shape[0] - 3
    measured_quantities = window[:ensemble_profiles].astype(jnp.float32)
    average = jnp.mean(measured_quantities, axis=0)
    deviation = measured_quantities - average
    innovation = window[ensemble_profiles].astype(jnp.float32) - average
    obs_precision = window[ensemble_profiles + 2].astype(jnp.float32) / window[
        ensemble_profiles + 1
    ].astype(jnp.float32)
    return (deviation, innovation, obs_precision)


def weights_for(deviation, innovation, precision, portions):
    ensemble_profiles = deviation.shape[0]
    portion_width = deviation.shape[1] // portions
    spread = jnp.zeros((ensemble_profiles, ensemble_profiles), jnp.float32)
    for portion_index in range(portions):
        portion = deviation[:, portion_index * portion_width : (portion_index + 1) * portion_width]
        scaled = (
            portion
            * precision[None, portion_index * portion_width : (portion_index + 1) * portion_width]
        )
        spread = spread + jnp.dot(
            scaled, portion.T, precision=EXACT, preferred_element_type=jnp.float32
        )
    spread = spread / (ensemble_profiles - 1.0)
    pulled = jnp.dot(
        deviation, precision * innovation, precision=EXACT, preferred_element_type=jnp.float32
    ) / (ensemble_profiles - 1.0)
    identity = jnp.eye(ensemble_profiles, dtype=jnp.float32)
    system = identity + spread
    norm_scale = jnp.sqrt(jnp.sum(system * system))

    def newton(sweep, carry):
        current, inv_root = carry
        middle = 1.5 * identity - 0.5 * jnp.dot(inv_root, current, precision=EXACT)
        return (
            jnp.dot(current, middle, precision=EXACT),
            jnp.dot(middle, inv_root, precision=EXACT),
        )

    current, inv_root = lax.fori_loop(0, NS_ITERS, newton, (system / norm_scale, identity))
    inv_root = inv_root / jnp.sqrt(norm_scale)
    inverse = jnp.dot(inv_root, inv_root, precision=EXACT)
    mean_weight = jnp.dot(inverse, pulled, precision=EXACT)
    return inv_root + mean_weight[:, None]


def update(states, transform, land_block):
    values = states.astype(jnp.float32)
    average = jnp.mean(values, axis=0)
    deviation = values - average[None]
    moved = jnp.einsum("isc,ij->jsc", deviation, transform, precision=EXACT)
    result = jnp.where(land_block[None, None, :] > 0, average[None] + moved, values)
    return result.astype(jnp.bfloat16)


def plain_on_device(
    ensemble_profiles_before,
    mixing_coefficient,
    surface_driver,
    terrain_indicator,
    measured_profile_position,
    measured_field_index,
    obs_valid,
    obs_value,
    obs_error,
    local_weight,
):
    background_ensemble = vertical_mixing_step(
        ensemble_profiles_before, mixing_coefficient, surface_driver, terrain_indicator
    )
    measured_quantities = measurement_operator(
        background_ensemble, measured_profile_position, measured_field_index
    )
    metadata = jnp.stack([obs_value, obs_error, obs_valid.astype(jnp.bfloat16)])
    own_rows = jnp.concatenate([measured_quantities, metadata], axis=0)
    pieces = []
    for offset in range(-REACH, REACH + 1):
        if offset == 0:
            pieces.append(own_rows)
        else:
            pieces.append(from_behind(own_rows, "tile", -offset))
    nearby = jnp.concatenate(pieces, axis=1)
    members_here = measured_quantities.shape[0]
    everyone = lax.all_gather(nearby[:members_here], "mem", axis=0, tiled=True)
    window = jnp.concatenate([everyone, nearby[members_here:]], axis=0)
    regrouped_states = lax.all_to_all(
        background_ensemble, "mem", split_axis=2, concat_axis=0, tiled=True
    )
    deviation, innovation, obs_precision = prepare(window)
    columns_here = regrouped_states.shape[2]
    local_land = lax.dynamic_slice_in_dim(
        terrain_indicator, lax.axis_index("mem") * columns_here, columns_here
    )
    transform = weights_for(
        deviation, innovation, obs_precision * local_weight[0, 0], 2 * REACH + 1
    )
    outputs = update(regrouped_states, transform, local_land)
    return lax.all_to_all(outputs, "mem", split_axis=0, concat_axis=2, tiled=True)


MESH = pl.DeviceIdType.MESH
HALVES = 2
FIELD_CUTS = (0.15, 0.5, 0.8)
CORES = 2


def exact_dot(a, b):
    return jnp.dot(a, b, precision=EXACT, preferred_element_type=jnp.float32)


def kernel(
    n_mem,
    n_tile,
    cuts,
    ens_hbm,
    mix_hbm,
    surf_hbm,
    land_hbm,
    pos_hbm,
    field_hbm,
    valid_hbm,
    value_hbm,
    error_hbm,
    weight_hbm,
    out_ref,
    ens_ref,
    mix_ref,
    surf_ref,
    land_ref,
    pos_ref,
    field_ref,
    valid_ref,
    value_ref,
    error_ref,
    fc_ref,
    seen_ref,
    near_ref,
    slot_ref,
    acc_ref,
    part_ref,
    got_ref,
    tsend_ref,
    trecv_ref,
    moved_ref,
    ens_sem,
    in_sem,
    seen_send,
    seen_recv,
    fc_send,
    fc_recv,
    w_send,
    w_recv,
    p_send,
    p_recv,
    t_send,
    t_recv,
):
    members, fields, columns = ens_ref.shape
    everyone = members * n_mem
    slots = pos_ref.shape[1]
    near = 2 * REACH + 1
    me, tile = lax.axis_index("mem"), lax.axis_index("tile")
    n_y = n_mem // CORES
    y, core = me // CORES, lax.rem(me, CORES)
    sibling = y * CORES + (1 - core)
    across = [lax.rem(y + step, n_y) * CORES + core for step in range(1, n_y)]
    partner_of = [lax.rem(y + step, n_y) * CORES + (1 - core) for step in range(1, n_y)]

    barrier = pltpu.get_barrier_semaphore()
    for step in range(1, n_mem):
        pl.semaphore_signal(
            barrier, inc=1, device_id={"mem": lax.rem(me + step, n_mem)}, device_id_type=MESH
        )
    for offset in range(-REACH, REACH + 1):
        if offset:
            pl.semaphore_signal(
                barrier,
                inc=1,
                device_id={"tile": lax.rem(tile + offset + n_tile, n_tile)},
                device_id_type=MESH,
            )

    lanes = 128

    def ens_copy(step):
        where = pl.ds(pl.multiple_of(step * lanes, lanes), lanes)
        return pltpu.make_async_copy(
            ens_hbm.at[:, :, where], ens_ref.at[:, :, where], ens_sem.at[step]
        )

    pairs = [
        (mix_hbm, mix_ref),
        (surf_hbm, surf_ref),
        (land_hbm, land_ref),
        (pos_hbm, pos_ref),
        (field_hbm, field_ref),
        (valid_hbm, valid_ref),
        (value_hbm, value_ref),
        (error_hbm, error_ref),
        (weight_hbm.at[REACH], near_ref.at[REACH]),
    ]
    inputs = [
        pltpu.make_async_copy(src, dst, in_sem.at[index]) for index, (src, dst) in enumerate(pairs)
    ]
    for copy in inputs[:3]:
        copy.start()
    for step in range(columns // lanes):
        ens_copy(step).start()
    for copy in inputs[3:]:
        copy.start()
    for copy in inputs[:3]:
        copy.wait()

    def mix(step, carry):
        where = pl.ds(pl.multiple_of(step * lanes, lanes), lanes)
        ens_copy(step).wait()
        x = jnp.transpose(ens_ref[:, :, where].astype(jnp.float32), (1, 0, 2))
        rate = mix_ref[:, where][None]
        above = jnp.concatenate([x[:1], x[:-1]], axis=0)
        below = jnp.concatenate([x[1:], x[-1:]], axis=0)
        stepped = x + rate * (above - 2.0 * x + below) - 0.05 * x * x * x
        top = stepped[:1] + surf_ref[:, where][None]
        stepped = jnp.concatenate([top, stepped[1:]], axis=0)
        land = jnp.broadcast_to(land_ref[:, where][None], x.shape) > 0
        fc_ref[me, :, :, where] = jnp.where(land, stepped, x).astype(jnp.bfloat16)
        return carry

    lax.fori_loop(0, columns // lanes, mix, 0)
    pl.semaphore_wait(barrier, n_mem - 1 + 2 * REACH)

    def remote(src, dst, send, recv, where):
        return pltpu.make_async_remote_copy(
            src_ref=src,
            dst_ref=dst,
            send_sem=send,
            recv_sem=recv,
            device_id=where,
            device_id_type=MESH,
        )

    started = []

    def go(copy):
        copy.start()
        started.append(copy)

    def weight_copy(j):
        return remote(
            weight_hbm.at[j],
            near_ref.at[j],
            w_send.at[j],
            w_recv.at[j],
            {"tile": lax.rem(tile + j - REACH + n_tile, n_tile)},
        )

    def fc_copy(q, owner, lane, target):
        block = fc_ref.at[owner, pl.ds(cuts[q], cuts[q + 1] - cuts[q])]
        return remote(block, block, fc_send.at[q, lane], fc_recv.at[q, owner], {"mem": target})

    def seen_copy(h, owner, lane, target):
        block = seen_ref.at[owner, h]
        return remote(
            block, block, seen_send.at[h, lane], seen_recv.at[h, owner], {"mem": target}
        )

    def own_fc(q):
        for index, peer in enumerate(across):
            go(fc_copy(q, me, index, peer))
        go(fc_copy(q, me, n_y - 1, sibling))

    def relay_fc(q):
        for index, peer in enumerate(across):
            fc_copy(q, peer, index, peer).wait_recv()
            go(fc_copy(q, peer, n_y + index, sibling))

    for j in range(near):
        if j != REACH:
            go(weight_copy(j))
    own_fc(0)

    for copy in inputs[3:]:
        copy.wait()
    half = slots // HALVES
    width = min(half, 512)
    for h in range(HALVES):

        def pick(step, carry, h=h):
            inner = pl.ds(pl.multiple_of(step * width, width), width)
            where = pl.ds(pl.multiple_of(h * half + step * width, width), width)
            rows = lax.broadcasted_iota(jnp.int32, (columns, width), 0)
            hot = jnp.where(rows == pos_ref[:, where], 1.0, 0.0).astype(jnp.bfloat16)
            flat = fc_ref[me].reshape(fields * members, columns)
            found = jnp.dot(flat, hot, preferred_element_type=jnp.float32)
            wanted = jnp.broadcast_to(field_ref[:, where], (members, width))
            total = found[:members]
            for f in range(1, fields):
                total = jnp.where(wanted == f, found[f * members : (f + 1) * members], total)
            seen_ref[me, h, :, inner] = total.astype(jnp.bfloat16)
            return carry

        lax.fori_loop(0, half // width, pick, 0)
        for index, peer in enumerate(across):
            go(seen_copy(h, me, index, peer))
        go(seen_copy(h, me, n_y - 1, sibling))

    n_cuts = len(cuts) - 1
    for q in range(1, n_cuts):
        own_fc(q)

    base = valid_ref[...].astype(jnp.float32) / error_ref[...].astype(jnp.float32)
    slot_ref[near] = value_ref[...].astype(jnp.float32)
    for spare in range(near + 1, slot_ref.shape[0]):
        slot_ref[spare] = jnp.zeros_like(base)
    for j in range(near):
        if j != REACH:
            weight_copy(j).wait_recv()
        slot_ref[j] = base * near_ref[j]
    acc_ref[...] = jnp.zeros_like(acc_ref)
    relay_fc(0)

    for h in range(HALVES):
        for index, peer in enumerate(across):
            seen_copy(h, peer, index, peer).wait_recv()
            go(seen_copy(h, peer, n_y + index, sibling))
    for h in range(HALVES):
        for owner in [sibling, *partner_of]:
            seen_copy(h, owner, 0, sibling).wait_recv()

        def gather_stats(step, carry, h=h):
            inner = pl.ds(pl.multiple_of(step * width, width), width)
            seen = jnp.concatenate(
                [seen_ref[m, h, :, inner].astype(jnp.float32) for m in range(n_mem)], axis=0
            )
            average = jnp.mean(seen, axis=0, keepdims=True)
            deviation = seen - average
            first = (h * half + step * width) // lanes
            rinv = jnp.concatenate(
                [slot_ref[:, first + r, :] for r in range(width // lanes)], axis=1
            )
            innovation = rinv[near : near + 1] - average
            high = deviation.astype(jnp.bfloat16)
            low = (deviation - high.astype(jnp.float32)).astype(jnp.bfloat16)
            right = jnp.concatenate([high, low], axis=0)
            pulls = rinv * innovation
            rows = [(deviation * rinv[j : j + 1]).astype(jnp.bfloat16) for j in range(near)]
            rows.append(jnp.concatenate([pulls, jnp.zeros_like(pulls)], axis=0).astype(jnp.bfloat16))
            left = jnp.concatenate(rows, axis=0)
            sums = lax.dot_general(
                left, right, (((1,), (1,)), ((), ())), preferred_element_type=jnp.float32
            )
            acc_ref[...] += sums
            return carry

        lax.fori_loop(0, half // width, gather_stats, 0)

    fold = everyone // 2
    for j in range(near):
        sums = acc_ref[j * everyone : (j + 1) * everyone]
        sums = sums[:, :everyone] + sums[:, everyone:]
        part_ref[j, :fold] = jnp.concatenate([sums[:fold], sums[fold:]], axis=1)
        part_ref[j, fold:] = jnp.broadcast_to(
            acc_ref[near * everyone + j : near * everyone + j + 1], (8, 2 * everyone)
        )

    def part_copy(j):
        return remote(
            part_ref.at[j],
            got_ref.at[j],
            p_send.at[j],
            p_recv.at[j],
            {"tile": lax.rem(tile - (j - REACH) + n_tile, n_tile)},
        )

    for j in range(near):
        if j != REACH:
            go(part_copy(j))
    for q in range(1, n_cuts - 2):
        relay_fc(q)
    summed = part_ref[REACH]
    for j in range(near):
        if j != REACH:
            part_copy(j).wait_recv()
            summed = summed + got_ref[j]
    summed = summed / (everyone - 1.0)
    spread = jnp.concatenate([summed[:fold, :everyone], summed[:fold, everyone:]], axis=0)
    pulled = summed[fold:, :everyone] + summed[fold:, everyone:]
    rows = lax.broadcasted_iota(jnp.int32, (everyone, everyone), 0)
    identity = jnp.where(
        rows == lax.broadcasted_iota(jnp.int32, (everyone, everyone), 1), 1.0, 0.0
    )
    system = identity + spread
    scale = jnp.sqrt(jnp.sum(system * system, keepdims=True))
    current = system / scale
    root = 1.5 * identity - 0.5 * current
    current = exact_dot(current, root)
    for sweep in range(1, NS_ITERS):
        middle = 1.5 * identity - 0.5 * exact_dot(root, current)
        if sweep < NS_ITERS - 1:
            current = exact_dot(current, middle)
        root = exact_dot(middle, root)
    root = root / jnp.sqrt(scale)
    mean_weight = exact_dot(exact_dot(pulled, root), root)[:1]
    turned = root + mean_weight
    turned = turned + (1.0 - jnp.sum(turned, axis=1, keepdims=True)) / everyone
    for m in range(n_mem):
        tsend_ref[m, :, :everyone] = turned[m * members : (m + 1) * members]
        tsend_ref[m, :, everyone:] = jnp.zeros((members, everyone), jnp.float32)

    def t_copy(owner, target, lane):
        return remote(
            tsend_ref.at[target],
            trecv_ref.at[owner],
            t_send.at[lane],
            t_recv.at[owner],
            {"mem": target},
        )

    for step in range(1, n_mem):
        go(t_copy(me, lax.rem(me + step, n_mem), step))
    trecv_ref[me] = tsend_ref[me]
    for q in range(n_cuts - 2, n_cuts):
        relay_fc(q)
    for q in range(n_cuts):
        for owner in [sibling, *partner_of]:
            fc_copy(q, owner, 0, sibling).wait_recv()
    for step in range(1, n_mem):
        t_copy(lax.rem(me + step, n_mem), me, step).wait_recv()

    wide = columns // n_mem
    group = 8

    def apply(block, carry):
        where = pl.ds(pl.multiple_of(block * wide, wide), wide)
        weights = trecv_ref[block][:, :everyone]
        high = weights.astype(jnp.bfloat16)
        low = (weights - high.astype(jnp.float32)).astype(jnp.bfloat16)
        left = jnp.concatenate([high, low], axis=0)
        land = jnp.broadcast_to(land_ref[:, where], (members, wide)) > 0
        for first in range(0, fields, group):
            states = jnp.concatenate(
                [
                    jnp.concatenate([fc_ref[m, f, :, where] for m in range(n_mem)], axis=0)
                    for f in range(first, first + group)
                ],
                axis=1,
            )
            both = jnp.dot(left, states, preferred_element_type=jnp.float32)
            total = both[:members] + both[members:]
            for f in range(group):
                moved_ref[first + f, :, :] = jnp.where(
                    land,
                    total[:, f * wide : (f + 1) * wide],
                    fc_ref[me, first + f, :, where].astype(jnp.float32),
                )
        out_ref[:, :, where] = jnp.transpose(moved_ref[...], (1, 0, 2)).astype(jnp.bfloat16)
        return carry

    lax.fori_loop(0, n_mem, apply, 0)
    for copy in started:
        copy.wait_send()


def on_device(
    n_mem,
    n_tile,
    ensemble_profiles_before,
    mixing_coefficient,
    surface_driver,
    terrain_indicator,
    measured_profile_position,
    measured_field_index,
    obs_valid,
    obs_value,
    obs_error,
    local_weight,
):
    members, fields, columns = ensemble_profiles_before.shape
    slots = measured_field_index.shape[0]
    everyone = members * n_mem
    near = 2 * REACH + 1
    n_y = n_mem // CORES
    cuts = (0, *[int(fields * cut) for cut in FIELD_CUTS], fields)
    n_cuts = len(cuts) - 1
    row = lambda a: a.reshape(1, -1)
    table = lambda a: a.reshape(-1, 128)
    far = pl.BlockSpec(memory_space=pltpu.HBM)
    dma = pltpu.SemaphoreType.DMA
    return pl.pallas_call(
        functools.partial(kernel, n_mem, n_tile, cuts),
        out_shape=jax.ShapeDtypeStruct(ensemble_profiles_before.shape, jnp.bfloat16),
        in_specs=[far] * 10,
        out_specs=pl.BlockSpec(memory_space=pltpu.VMEM),
        scratch_shapes=[
            pltpu.VMEM((members, fields, columns), jnp.bfloat16),
            pltpu.VMEM((1, columns), jnp.float32),
            pltpu.VMEM((members, columns), jnp.float32),
            pltpu.VMEM((1, columns), jnp.int32),
            pltpu.VMEM((1, slots), jnp.int32),
            pltpu.VMEM((1, slots), jnp.int32),
            pltpu.VMEM((slots // 128, 128), jnp.int32),
            pltpu.VMEM((slots // 128, 128), jnp.bfloat16),
            pltpu.VMEM((slots // 128, 128), jnp.bfloat16),
            pltpu.VMEM((n_mem, fields, members, columns), jnp.bfloat16),
            pltpu.VMEM((n_mem, HALVES, members, slots // HALVES), jnp.bfloat16),
            pltpu.VMEM((near, slots // 128, 128), jnp.float32),
            pltpu.VMEM((8, slots // 128, 128), jnp.float32),
            pltpu.VMEM((near * everyone + 16, 2 * everyone), jnp.float32),
            pltpu.VMEM((near, everyone // 2 + 8, 2 * everyone), jnp.float32),
            pltpu.VMEM((near, everyone // 2 + 8, 2 * everyone), jnp.float32),
            pltpu.VMEM((n_mem, members, 2 * everyone), jnp.float32),
            pltpu.VMEM((n_mem, members, 2 * everyone), jnp.float32),
            pltpu.VMEM((fields, members, columns // n_mem), jnp.float32),
            dma((columns // 128,)),
            dma((9,)),
            dma((HALVES, 2 * n_y)),
            dma((HALVES, n_mem)),
            dma((n_cuts, 2 * n_y)),
            dma((n_cuts, n_mem)),
            dma((near,)),
            dma((near,)),
            dma((near,)),
            dma((near,)),
            dma((n_mem,)),
            dma((n_mem,)),
        ],
        compiler_params=pltpu.CompilerParams(
            collective_id=0, has_side_effects=True, vmem_limit_bytes=48 * 2**20
        ),
    )(
        ensemble_profiles_before,
        row(mixing_coefficient),
        surface_driver,
        row(terrain_indicator),
        row(measured_profile_position),
        row(measured_field_index),
        table(obs_valid),
        table(obs_value),
        table(obs_error),
        local_weight.reshape(near, slots // 128, 128),
    )


def fits(n_mem, n_tile, ensemble, slots):
    members, fields, columns = ensemble[0] // n_mem, ensemble[1], ensemble[2] // n_tile
    return (
        n_mem % CORES == 0
        and n_tile > 2 * REACH
        and members % 16 == 0
        and fields % 8 == 0
        and columns % (128 * n_mem) == 0
        and slots // n_tile % (512 * HALVES) == 0
    )


def solution(mesh):
    in_specs = (
        P("mem", None, "tile"),
        P("tile"),
        P("mem", "tile"),
        P("tile"),
        P("tile"),
        P("tile"),
        P("tile"),
        P("tile"),
        P("tile"),
        P("mem", "tile", None),
    )
    out_specs = P("mem", None, "tile")

    def run(*args):
        sizes = mesh.shape["mem"], mesh.shape["tile"]
        body = plain_on_device
        if fits(*sizes, args[0].shape, args[5].shape[0]):
            body = functools.partial(on_device, *sizes)
        return jax.shard_map(
            body, mesh=mesh, in_specs=in_specs, out_specs=out_specs, check_vma=False
        )(*args)

    return run
```

```python
import functools

import jax
import jax.numpy as jnp
from jax import lax
from jax.experimental import pallas as pl
from jax.experimental.pallas import tpu as pltpu
from jax.sharding import PartitionSpec as P

REACH = 2
NS_ITERS = 3


EXACT = lax.Precision.HIGHEST


def from_behind(value, axis, steps):
    count = lax.axis_size(axis)
    pairs = [(source, (source + steps) % count) for source in range(count)]
    return lax.ppermute(value, axis, pairs)


def vertical_mixing_step(
    ensemble_profiles_before, mixing_coefficient, surface_driver, terrain_indicator
):
    values = ensemble_profiles_before.astype(jnp.float32)
    above_layer = jnp.concatenate([values[:, :1], values[:, :-1]], axis=1)
    below_layer = jnp.concatenate([values[:, 1:], values[:, -1:]], axis=1)
    diffused = values + mixing_coefficient[None, None, :] * (
        above_layer - 2.0 * values + below_layer
    )
    stepped = diffused - 0.05 * values * values * values
    surface = jnp.concatenate([stepped[:, :1] + surface_driver[:, None, :], stepped[:, 1:]], axis=1)
    result = jnp.where(terrain_indicator[None, None, :] > 0, surface, values)
    return result.astype(jnp.bfloat16)


def measurement_operator(background_ensemble, measured_profile_position, measured_field_index):
    profile_sequence = background_ensemble.shape[2]
    unrolled_ensemble = background_ensemble.reshape(background_ensemble.shape[0], -1)
    slot_index = measured_field_index * profile_sequence + measured_profile_position
    return jnp.take(unrolled_ensemble, slot_index, axis=1)


def prepare(window):
    ensemble_profiles = window.shape[0] - 3
    measured_quantities = window[:ensemble_profiles].astype(jnp.float32)
    average = jnp.mean(measured_quantities, axis=0)
    deviation = measured_quantities - average
    innovation = window[ensemble_profiles].astype(jnp.float32) - average
    obs_precision = window[ensemble_profiles + 2].astype(jnp.float32) / window[
        ensemble_profiles + 1
    ].astype(jnp.float32)
    return (deviation, innovation, obs_precision)


def weights_for(deviation, innovation, precision, portions):
    ensemble_profiles = deviation.shape[0]
    portion_width = deviation.shape[1] // portions
    spread = jnp.zeros((ensemble_profiles, ensemble_profiles), jnp.float32)
    for portion_index in range(portions):
        portion = deviation[:, portion_index * portion_width : (portion_index + 1) * portion_width]
        scaled = (
            portion
            * precision[None, portion_index * portion_width : (portion_index + 1) * portion_width]
        )
        spread = spread + jnp.dot(
            scaled, portion.T, precision=EXACT, preferred_element_type=jnp.float32
        )
    spread = spread / (ensemble_profiles - 1.0)
    pulled = jnp.dot(
        deviation, precision * innovation, precision=EXACT, preferred_element_type=jnp.float32
    ) / (ensemble_profiles - 1.0)
    identity = jnp.eye(ensemble_profiles, dtype=jnp.float32)
    system = identity + spread
    norm_scale = jnp.sqrt(jnp.sum(system * system))

    def newton(sweep, carry):
        current, inv_root = carry
        middle = 1.5 * identity - 0.5 * jnp.dot(inv_root, current, precision=EXACT)
        return (
            jnp.dot(current, middle, precision=EXACT),
            jnp.dot(middle, inv_root, precision=EXACT),
        )

    current, inv_root = lax.fori_loop(0, NS_ITERS, newton, (system / norm_scale, identity))
    inv_root = inv_root / jnp.sqrt(norm_scale)
    inverse = jnp.dot(inv_root, inv_root, precision=EXACT)
    mean_weight = jnp.dot(inverse, pulled, precision=EXACT)
    return inv_root + mean_weight[:, None]


def update(states, transform, land_block):
    values = states.astype(jnp.float32)
    average = jnp.mean(values, axis=0)
    deviation = values - average[None]
    moved = jnp.einsum("isc,ij->jsc", deviation, transform, precision=EXACT)
    result = jnp.where(land_block[None, None, :] > 0, average[None] + moved, values)
    return result.astype(jnp.bfloat16)


def plain_on_device(
    ensemble_profiles_before,
    mixing_coefficient,
    surface_driver,
    terrain_indicator,
    measured_profile_position,
    measured_field_index,
    obs_valid,
    obs_value,
    obs_error,
    local_weight,
):
    background_ensemble = vertical_mixing_step(
        ensemble_profiles_before, mixing_coefficient, surface_driver, terrain_indicator
    )
    measured_quantities = measurement_operator(
        background_ensemble, measured_profile_position, measured_field_index
    )
    metadata = jnp.stack([obs_value, obs_error, obs_valid.astype(jnp.bfloat16)])
    own_rows = jnp.concatenate([measured_quantities, metadata], axis=0)
    pieces = []
    for offset in range(-REACH, REACH + 1):
        if offset == 0:
            pieces.append(own_rows)
        else:
            pieces.append(from_behind(own_rows, "tile", -offset))
    nearby = jnp.concatenate(pieces, axis=1)
    members_here = measured_quantities.shape[0]
    everyone = lax.all_gather(nearby[:members_here], "mem", axis=0, tiled=True)
    window = jnp.concatenate([everyone, nearby[members_here:]], axis=0)
    regrouped_states = lax.all_to_all(
        background_ensemble, "mem", split_axis=2, concat_axis=0, tiled=True
    )
    deviation, innovation, obs_precision = prepare(window)
    columns_here = regrouped_states.shape[2]
    local_land = lax.dynamic_slice_in_dim(
        terrain_indicator, lax.axis_index("mem") * columns_here, columns_here
    )
    transform = weights_for(
        deviation, innovation, obs_precision * local_weight[0, 0], 2 * REACH + 1
    )
    outputs = update(regrouped_states, transform, local_land)
    return lax.all_to_all(outputs, "mem", split_axis=0, concat_axis=2, tiled=True)


MESH = pl.DeviceIdType.MESH
HALVES = 2
FIELD_CUTS = (0.25, 0.5, 0.8)
CORES = 2


def exact_dot(a, b):
    return jnp.dot(a, b, precision=EXACT, preferred_element_type=jnp.float32)


def kernel(
    n_mem,
    n_tile,
    cuts,
    ens_hbm,
    mix_hbm,
    surf_hbm,
    land_hbm,
    pos_hbm,
    field_hbm,
    valid_hbm,
    value_hbm,
    error_hbm,
    weight_hbm,
    out_ref,
    ens_ref,
    mix_ref,
    surf_ref,
    land_ref,
    pos_ref,
    field_ref,
    valid_ref,
    value_ref,
    error_ref,
    fc_ref,
    seen_ref,
    near_ref,
    slot_ref,
    acc_ref,
    part_ref,
    got_ref,
    tsend_ref,
    trecv_ref,
    moved_ref,
    ens_sem,
    in_sem,
    seen_send,
    seen_recv,
    fc_send,
    fc_recv,
    w_send,
    w_recv,
    p_send,
    p_recv,
    t_send,
    t_recv,
):
    members, fields, columns = ens_ref.shape
    everyone = members * n_mem
    slots = pos_ref.shape[1]
    near = 2 * REACH + 1
    me, tile = lax.axis_index("mem"), lax.axis_index("tile")
    n_y = n_mem // CORES
    y, core = me // CORES, lax.rem(me, CORES)
    sibling = y * CORES + (1 - core)
    across = [lax.rem(y + step, n_y) * CORES + core for step in range(1, n_y)]
    partner_of = [lax.rem(y + step, n_y) * CORES + (1 - core) for step in range(1, n_y)]

    barrier = pltpu.get_barrier_semaphore()
    for step in range(1, n_mem):
        pl.semaphore_signal(
            barrier, inc=1, device_id={"mem": lax.rem(me + step, n_mem)}, device_id_type=MESH
        )
    for offset in range(-REACH, REACH + 1):
        if offset:
            pl.semaphore_signal(
                barrier,
                inc=1,
                device_id={"tile": lax.rem(tile + offset + n_tile, n_tile)},
                device_id_type=MESH,
            )

    lanes = 128

    def ens_copy(step):
        where = pl.ds(pl.multiple_of(step * lanes, lanes), lanes)
        return pltpu.make_async_copy(
            ens_hbm.at[:, :, where], ens_ref.at[:, :, where], ens_sem.at[step]
        )

    pairs = [
        (mix_hbm, mix_ref),
        (surf_hbm, surf_ref),
        (land_hbm, land_ref),
        (pos_hbm, pos_ref),
        (field_hbm, field_ref),
        (valid_hbm, valid_ref),
        (value_hbm, value_ref),
        (error_hbm, error_ref),
        (weight_hbm.at[REACH], near_ref.at[REACH]),
    ]
    inputs = [
        pltpu.make_async_copy(src, dst, in_sem.at[index]) for index, (src, dst) in enumerate(pairs)
    ]
    for copy in inputs[:3]:
        copy.start()
    for step in range(columns // lanes):
        ens_copy(step).start()
    for copy in inputs[3:]:
        copy.start()
    for copy in inputs[:3]:
        copy.wait()

    def mix(step, carry):
        where = pl.ds(pl.multiple_of(step * lanes, lanes), lanes)
        ens_copy(step).wait()
        x = jnp.transpose(ens_ref[:, :, where].astype(jnp.float32), (1, 0, 2))
        rate = mix_ref[:, where][None]
        above = jnp.concatenate([x[:1], x[:-1]], axis=0)
        below = jnp.concatenate([x[1:], x[-1:]], axis=0)
        stepped = x + rate * (above - 2.0 * x + below) - 0.05 * x * x * x
        top = stepped[:1] + surf_ref[:, where][None]
        stepped = jnp.concatenate([top, stepped[1:]], axis=0)
        land = jnp.broadcast_to(land_ref[:, where][None], x.shape) > 0
        fc_ref[me, :, :, where] = jnp.where(land, stepped, x).astype(jnp.bfloat16)
        return carry

    lax.fori_loop(0, columns // lanes, mix, 0)
    pl.semaphore_wait(barrier, n_mem - 1 + 2 * REACH)

    def remote(src, dst, send, recv, where):
        return pltpu.make_async_remote_copy(
            src_ref=src,
            dst_ref=dst,
            send_sem=send,
            recv_sem=recv,
            device_id=where,
            device_id_type=MESH,
        )

    started = []

    def go(copy):
        copy.start()
        started.append(copy)

    def weight_copy(j):
        return remote(
            weight_hbm.at[j],
            near_ref.at[j],
            w_send.at[j],
            w_recv.at[j],
            {"tile": lax.rem(tile + j - REACH + n_tile, n_tile)},
        )

    def fc_copy(q, owner, lane, target):
        block = fc_ref.at[owner, pl.ds(cuts[q], cuts[q + 1] - cuts[q])]
        return remote(block, block, fc_send.at[q, lane], fc_recv.at[q, owner], {"mem": target})

    def seen_copy(h, owner, lane, target):
        block = seen_ref.at[owner, h]
        return remote(
            block, block, seen_send.at[h, lane], seen_recv.at[h, owner], {"mem": target}
        )

    def own_fc(q):
        for index, peer in enumerate(across):
            go(fc_copy(q, me, index, peer))
        go(fc_copy(q, me, n_y - 1, sibling))

    def relay_fc(q):
        for index, peer in enumerate(across):
            fc_copy(q, peer, index, peer).wait_recv()
            go(fc_copy(q, peer, n_y + index, sibling))

    for j in range(near):
        if j != REACH:
            go(weight_copy(j))
    own_fc(0)

    for copy in inputs[3:]:
        copy.wait()
    half = slots // HALVES
    width = min(half, 512)
    for h in range(HALVES):

        def pick(step, carry, h=h):
            inner = pl.ds(pl.multiple_of(step * width, width), width)
            where = pl.ds(pl.multiple_of(h * half + step * width, width), width)
            rows = lax.broadcasted_iota(jnp.int32, (columns, width), 0)
            hot = jnp.where(rows == pos_ref[:, where], 1.0, 0.0).astype(jnp.bfloat16)
            flat = fc_ref[me].reshape(fields * members, columns)
            found = jnp.dot(flat, hot, preferred_element_type=jnp.float32)
            wanted = jnp.broadcast_to(field_ref[:, where], (members, width))
            total = found[:members]
            for f in range(1, fields):
                total = jnp.where(wanted == f, found[f * members : (f + 1) * members], total)
            seen_ref[me, h, :, inner] = total.astype(jnp.bfloat16)
            return carry

        lax.fori_loop(0, half // width, pick, 0)
        for index, peer in enumerate(across):
            go(seen_copy(h, me, index, peer))
        go(seen_copy(h, me, n_y - 1, sibling))

    n_cuts = len(cuts) - 1
    for q in range(1, n_cuts):
        own_fc(q)

    base = valid_ref[...].astype(jnp.float32) / error_ref[...].astype(jnp.float32)
    slot_ref[near] = value_ref[...].astype(jnp.float32)
    for spare in range(near + 1, slot_ref.shape[0]):
        slot_ref[spare] = jnp.zeros_like(base)
    for j in range(near):
        if j != REACH:
            weight_copy(j).wait_recv()
        slot_ref[j] = base * near_ref[j]
    acc_ref[...] = jnp.zeros_like(acc_ref)
    relay_fc(0)

    for h in range(HALVES):
        for index, peer in enumerate(across):
            seen_copy(h, peer, index, peer).wait_recv()
            go(seen_copy(h, peer, n_y + index, sibling))
    for h in range(HALVES):
        for owner in [sibling, *partner_of]:
            seen_copy(h, owner, 0, sibling).wait_recv()

        def gather_stats(step, carry, h=h):
            inner = pl.ds(pl.multiple_of(step * width, width), width)
            seen = jnp.concatenate(
                [seen_ref[m, h, :, inner].astype(jnp.float32) for m in range(n_mem)], axis=0
            )
            average = jnp.mean(seen, axis=0, keepdims=True)
            deviation = seen - average
            first = (h * half + step * width) // lanes
            rinv = jnp.concatenate(
                [slot_ref[:, first + r, :] for r in range(width // lanes)], axis=1
            )
            innovation = rinv[near : near + 1] - average
            high = deviation.astype(jnp.bfloat16)
            low = (deviation - high.astype(jnp.float32)).astype(jnp.bfloat16)
            right = jnp.concatenate([high, low], axis=0)
            pulls = rinv * innovation
            rows = [(deviation * rinv[j : j + 1]).astype(jnp.bfloat16) for j in range(near)]
            rows.append(jnp.concatenate([pulls, jnp.zeros_like(pulls)], axis=0).astype(jnp.bfloat16))
            left = jnp.concatenate(rows, axis=0)
            sums = lax.dot_general(
                left, right, (((1,), (1,)), ((), ())), preferred_element_type=jnp.float32
            )
            acc_ref[...] += sums
            return carry

        lax.fori_loop(0, half // width, gather_stats, 0)

    fold = everyone // 2
    for j in range(near):
        sums = acc_ref[j * everyone : (j + 1) * everyone]
        sums = sums[:, :everyone] + sums[:, everyone:]
        part_ref[j, :fold] = jnp.concatenate([sums[:fold], sums[fold:]], axis=1)
        part_ref[j, fold:] = jnp.broadcast_to(
            acc_ref[near * everyone + j : near * everyone + j + 1], (8, 2 * everyone)
        )

    def part_copy(j):
        return remote(
            part_ref.at[j],
            got_ref.at[j],
            p_send.at[j],
            p_recv.at[j],
            {"tile": lax.rem(tile - (j - REACH) + n_tile, n_tile)},
        )

    for j in range(near):
        if j != REACH:
            go(part_copy(j))
    for q in range(1, n_cuts - 2):
        relay_fc(q)
    summed = part_ref[REACH]
    for j in range(near):
        if j != REACH:
            part_copy(j).wait_recv()
            summed = summed + got_ref[j]
    summed = summed / (everyone - 1.0)
    spread = jnp.concatenate([summed[:fold, :everyone], summed[:fold, everyone:]], axis=0)
    pulled = summed[fold:, :everyone] + summed[fold:, everyone:]
    rows = lax.broadcasted_iota(jnp.int32, (everyone, everyone), 0)
    identity = jnp.where(
        rows == lax.broadcasted_iota(jnp.int32, (everyone, everyone), 1), 1.0, 0.0
    )
    system = identity + spread
    scale = jnp.sqrt(jnp.sum(system * system, keepdims=True))
    current = system / scale
    root = 1.5 * identity - 0.5 * current
    current = exact_dot(current, root)
    for sweep in range(1, NS_ITERS):
        middle = 1.5 * identity - 0.5 * exact_dot(root, current)
        if sweep < NS_ITERS - 1:
            current = exact_dot(current, middle)
        root = exact_dot(middle, root)
    root = root / jnp.sqrt(scale)
    mean_weight = exact_dot(exact_dot(pulled, root), root)[:1]
    turned = root + mean_weight
    turned = turned + (1.0 - jnp.sum(turned, axis=1, keepdims=True)) / everyone
    for m in range(n_mem):
        tsend_ref[m, :, :everyone] = turned[m * members : (m + 1) * members]
        tsend_ref[m, :, everyone:] = jnp.zeros((members, everyone), jnp.float32)

    def t_copy(owner, target, lane):
        return remote(
            tsend_ref.at[target],
            trecv_ref.at[owner],
            t_send.at[lane],
            t_recv.at[owner],
            {"mem": target},
        )

    for step in range(1, n_mem):
        go(t_copy(me, lax.rem(me + step, n_mem), step))
    trecv_ref[me] = tsend_ref[me]
    for q in range(n_cuts - 2, n_cuts):
        relay_fc(q)
    for q in range(n_cuts):
        for owner in [sibling, *partner_of]:
            fc_copy(q, owner, 0, sibling).wait_recv()
    for step in range(1, n_mem):
        t_copy(lax.rem(me + step, n_mem), me, step).wait_recv()

    wide = columns // n_mem
    group = 8

    def apply(block, carry):
        where = pl.ds(pl.multiple_of(block * wide, wide), wide)
        weights = trecv_ref[block][:, :everyone]
        high = weights.astype(jnp.bfloat16)
        low = (weights - high.astype(jnp.float32)).astype(jnp.bfloat16)
        left = jnp.concatenate([high, low], axis=0)
        land = jnp.broadcast_to(land_ref[:, where], (members, wide)) > 0
        for first in range(0, fields, group):
            states = jnp.concatenate(
                [
                    jnp.concatenate([fc_ref[m, f, :, where] for m in range(n_mem)], axis=0)
                    for f in range(first, first + group)
                ],
                axis=1,
            )
            both = jnp.dot(left, states, preferred_element_type=jnp.float32)
            total = both[:members] + both[members:]
            for f in range(group):
                moved_ref[first + f, :, :] = jnp.where(
                    land,
                    total[:, f * wide : (f + 1) * wide],
                    fc_ref[me, first + f, :, where].astype(jnp.float32),
                )
        out_ref[:, :, where] = jnp.transpose(moved_ref[...], (1, 0, 2)).astype(jnp.bfloat16)
        return carry

    lax.fori_loop(0, n_mem, apply, 0)
    for copy in started:
        copy.wait_send()


def on_device(
    n_mem,
    n_tile,
    ensemble_profiles_before,
    mixing_coefficient,
    surface_driver,
    terrain_indicator,
    measured_profile_position,
    measured_field_index,
    obs_valid,
    obs_value,
    obs_error,
    local_weight,
):
    members, fields, columns = ensemble_profiles_before.shape
    slots = measured_field_index.shape[0]
    everyone = members * n_mem
    near = 2 * REACH + 1
    n_y = n_mem // CORES
    cuts = (0, *[int(fields * cut) for cut in FIELD_CUTS], fields)
    n_cuts = len(cuts) - 1
    row = lambda a: a.reshape(1, -1)
    table = lambda a: a.reshape(-1, 128)
    far = pl.BlockSpec(memory_space=pltpu.HBM)
    dma = pltpu.SemaphoreType.DMA
    return pl.pallas_call(
        functools.partial(kernel, n_mem, n_tile, cuts),
        out_shape=pltpu.VMEM(ensemble_profiles_before.shape, jnp.bfloat16),
        in_specs=[far] * 10,
        out_specs=pl.BlockSpec(memory_space=pltpu.VMEM),
        scratch_shapes=[
            pltpu.VMEM((members, fields, columns), jnp.bfloat16),
            pltpu.VMEM((1, columns), jnp.float32),
            pltpu.VMEM((members, columns), jnp.float32),
            pltpu.VMEM((1, columns), jnp.int32),
            pltpu.VMEM((1, slots), jnp.int32),
            pltpu.VMEM((1, slots), jnp.int32),
            pltpu.VMEM((slots // 128, 128), jnp.int32),
            pltpu.VMEM((slots // 128, 128), jnp.bfloat16),
            pltpu.VMEM((slots // 128, 128), jnp.bfloat16),
            pltpu.VMEM((n_mem, fields, members, columns), jnp.bfloat16),
            pltpu.VMEM((n_mem, HALVES, members, slots // HALVES), jnp.bfloat16),
            pltpu.VMEM((near, slots // 128, 128), jnp.float32),
            pltpu.VMEM((8, slots // 128, 128), jnp.float32),
            pltpu.VMEM((near * everyone + 16, 2 * everyone), jnp.float32),
            pltpu.VMEM((near, everyone // 2 + 8, 2 * everyone), jnp.float32),
            pltpu.VMEM((near, everyone // 2 + 8, 2 * everyone), jnp.float32),
            pltpu.VMEM((n_mem, members, 2 * everyone), jnp.float32),
            pltpu.VMEM((n_mem, members, 2 * everyone), jnp.float32),
            pltpu.VMEM((fields, members, columns // n_mem), jnp.float32),
            dma((columns // 128,)),
            dma((9,)),
            dma((HALVES, 2 * n_y)),
            dma((HALVES, n_mem)),
            dma((n_cuts, 2 * n_y)),
            dma((n_cuts, n_mem)),
            dma((near,)),
            dma((near,)),
            dma((near,)),
            dma((near,)),
            dma((n_mem,)),
            dma((n_mem,)),
        ],
        compiler_params=pltpu.CompilerParams(
            collective_id=0, has_side_effects=True, vmem_limit_bytes=66_000_000
        ),
    )(
        ensemble_profiles_before,
        row(mixing_coefficient),
        surface_driver,
        row(terrain_indicator),
        row(measured_profile_position),
        row(measured_field_index),
        table(obs_valid),
        table(obs_value),
        table(obs_error),
        local_weight.reshape(near, slots // 128, 128),
    )


def fits(n_mem, n_tile, ensemble, slots):
    members, fields, columns = ensemble[0] // n_mem, ensemble[1], ensemble[2] // n_tile
    return (
        n_mem % CORES == 0
        and n_tile > 2 * REACH
        and members % 16 == 0
        and fields % 8 == 0
        and columns % (128 * n_mem) == 0
        and slots // n_tile % (512 * HALVES) == 0
    )


def solution(mesh):
    in_specs = (
        P("mem", None, "tile"),
        P("tile"),
        P("mem", "tile"),
        P("tile"),
        P("tile"),
        P("tile"),
        P("tile"),
        P("tile"),
        P("tile"),
        P("mem", "tile", None),
    )
    out_specs = P("mem", None, "tile")

    def run(*args):
        sizes = mesh.shape["mem"], mesh.shape["tile"]
        body = plain_on_device
        if fits(*sizes, args[0].shape, args[5].shape[0]):
            body = functools.partial(on_device, *sizes)
        return jax.shard_map(
            body, mesh=mesh, in_specs=in_specs, out_specs=out_specs, check_vma=False
        )(*args)

    return run
```
